16 devices in a mesh: req: 2 (over y, z), cp: 8 (over x, core).
Axes of the slice: x: 4, y: 2, z: 1, core: 2. Of those that a mesh axis runs over, the one named last changes fastest.
The devices are a block of a 4x4x8 slice.
Arguments:
- x: bfloat16 [12288, 2048], P(('req', 'cp')), parts along dimension 0
- pos: int32 [12288], P(('req', 'cp')), parts along dimension 0
- g1: bfloat16 [2, 2048], replicated
- g2: bfloat16 [2, 2048], replicated
- wq: bfloat16 [2, 2048, 2048], replicated
- wk: bfloat16 [2, 2048, 2048], replicated
- wv: bfloat16 [2, 2048, 2048], replicated
- wo: bfloat16 [2, 2048, 2048], replicated
- w1: bfloat16 [2, 2048, 8192], replicated
- w3: bfloat16 [2, 2048, 8192], replicated
- w2: bfloat16 [2, 8192, 2048], replicated
Outputs:
- output 1: bfloat16 [12288, 2048], P(('req', 'cp')), parts along dimension 0
- output 2: bfloat16 [2, 12288, 16, 128], P(None, 'req', 'cp'), parts along dimension 1
- output 3: bfloat16 [2, 12288, 16, 128], P(None, 'req', 'cp'), parts along dimension 1
There are 2 independent parts. The reference program is written for one: setup_inputs(seed, part) draws one part's arguments, and reference() takes and returns one part's arrays. A program takes and returns all parts, laid end to end along the dimension named above; an argument that names none is the same for every part.
All inputs are finite; a program needn't handle non-finite values.
Results may differ from the reference program's by a relative error of at most 0.0178628.
Values are sent between devices in bfloat16 or wider.
A program may use at most 768 MiB of HBM per device.

```python
import jax
import jax.numpy as jnp
from jax import lax
import numpy as np

D = 2048
HEADS = 16
HEAD = 128
FF = 8192
LAYERS = 2
S_DEV = 768
CP = 8

SEQ = CP * S_DEV
SEG = S_DEV // 2


def _layout():
    rows = [np.arange(c * SEG, (c + 1) * SEG) for i in range(CP) for c in (i, 2 * CP - 1 - i)]
    return np.concatenate(rows).astype(np.int32)


def setup_inputs(seed: int = 0, part: int = 0) -> dict:
    key = jax.random.PRNGKey(seed)
    kx, ko = jax.random.split(jax.random.fold_in(key, part))
    ks = jax.random.split(key, 9)
    hd = HEADS * HEAD

    def w(k, shape, scale):
        return (jax.random.normal(k, shape, jnp.float32) * scale).astype(jnp.bfloat16)

    def gain(k):
        return (1.0 + 0.2 * jax.random.normal(k, (LAYERS, D), jnp.float32)).astype(jnp.bfloat16)

    p0 = jax.random.randint(ko, (), 0, 4096, jnp.int32)
    return {
        "x": jax.random.normal(kx, (SEQ, D), jnp.float32).astype(jnp.bfloat16),
        "pos": p0 + jnp.asarray(_layout()),
        "g1": gain(ks[0]),
        "g2": gain(ks[1]),
        "wq": w(ks[2], (LAYERS, D, hd), 1.7 * D ** -0.5),
        "wk": w(ks[3], (LAYERS, D, hd), 1.7 * D ** -0.5),
        "wv": w(ks[4], (LAYERS, D, hd), D ** -0.5),
        "wo": w(ks[5], (LAYERS, hd, D), hd ** -0.5),
        "w1": w(ks[6], (LAYERS, D, FF), D ** -0.5),
        "w3": w(ks[7], (LAYERS, D, FF), D ** -0.5),
        "w2": w(ks[8], (LAYERS, FF, D), FF ** -0.5),
    }


def _norm(x, g):
    x32 = x.astype(jnp.float32)
    r = lax.rsqrt(jnp.mean(x32 * x32, axis=-1, keepdims=True) + 1e-5)
    return (x32 * r * g.astype(jnp.float32)).astype(jnp.bfloat16)


def _rope(t, pos):
    half = HEAD // 2
    inv = 1.0 / (10000.0 ** (jnp.arange(half, dtype=jnp.float32) * (2.0 / HEAD)))
    ang = pos.astype(jnp.float32)[:, None] * inv[None, :]
    c = jnp.cos(ang)[:, None, :]
    s = jnp.sin(ang)[:, None, :]
    t1, t2 = t[..., :half], t[..., half:]
    return jnp.concatenate([t1 * c - t2 * s, t2 * c + t1 * s], axis=-1)


def _attention(q, k, v, pos):
    nb = SEQ // SEG
    scale = HEAD ** -0.5

    def head(a):
        qh, kh, vh = a

        def blk(b):
            qb, pb = b
            s = jnp.dot(qb, kh.T, preferred_element_type=jnp.float32) * scale
            s = jnp.where(pos[None, :] <= pb[:, None], s, -jnp.inf)
            p = jax.nn.softmax(s, axis=-1).astype(jnp.bfloat16)
            return jnp.dot(p, vh, preferred_element_type=jnp.float32).astype(jnp.bfloat16)

        o = lax.map(blk, (qh.reshape(nb, SEG, HEAD), pos.reshape(nb, SEG)))
        return o.reshape(SEQ, HEAD)

    o = lax.map(head, (q.transpose(1, 0, 2), k.transpose(1, 0, 2), v.transpose(1, 0, 2)))
    return o.transpose(1, 0, 2).reshape(SEQ, HEADS * HEAD)


def reference(x, pos, g1, g2, wq, wk, wv, wo, w1, w3, w2):
    order = jnp.argsort(pos)

    def layer(x, w):
        a1, a2, bq, bk, bv, bo, b1, b3, b2 = w
        h = _norm(x, a1)
        q = _rope(jnp.dot(h, bq, preferred_element_type=jnp.float32).reshape(SEQ, HEADS, HEAD), pos).astype(jnp.bfloat16)
        k = _rope(jnp.dot(h, bk, preferred_element_type=jnp.float32).reshape(SEQ, HEADS, HEAD), pos).astype(jnp.bfloat16)
        v = jnp.dot(h, bv, preferred_element_type=jnp.float32).astype(jnp.bfloat16).reshape(SEQ, HEADS, HEAD)
        o = _attention(q, k, v, pos)
        x = (x.astype(jnp.float32) + jnp.dot(o, bo, preferred_element_type=jnp.float32)).astype(jnp.bfloat16)
        h2 = _norm(x, a2)
        u = (jax.nn.silu(jnp.dot(h2, b1, preferred_element_type=jnp.float32))
             * jnp.dot(h2, b3, preferred_element_type=jnp.float32)).astype(jnp.bfloat16)
        x = (x.astype(jnp.float32) + jnp.dot(u, b2, preferred_element_type=jnp.float32)).astype(jnp.bfloat16)
        return x, (k[order], v[order])

    y, (kc, vc) = lax.scan(layer, x, (g1, g2, wq, wk, wv, wo, w1, w3, w2))
    return y, kc, vc
```

```python
import functools

import jax
import jax.numpy as jnp
from jax import lax
from jax.experimental import pallas as pl
from jax.experimental.pallas import tpu as pltpu
from jax.sharding import PartitionSpec as P

HEAD = 128
F32 = jnp.float32
BF16 = jnp.bfloat16
LOG2E = 1.4426950408889634
MESH = pl.DeviceIdType.MESH
HBM = pl.BlockSpec(memory_space=pltpu.HBM)


class _Exchange:
    def __init__(self, ncp, srcs, dsts, scratch, first, second, last):
        self.ncp, self.srcs, self.dsts = ncp, srcs, dsts
        self.ssem, self.rsem, self.lsem, self.own = scratch
        self.first, self.second, self.last = first, second, last

    def _remote(self):
        me = lax.axis_index('cp')
        req = lax.axis_index('req')
        out = []
        for n, (s, d) in enumerate(zip(self.srcs, self.dsts)):
            for o in range(1, self.ncp):
                t = lax.rem(me + o, self.ncp)
                i = n * (self.ncp - 1) + o - 1
                out.append(pltpu.make_async_remote_copy(
                    s.at[t], d.at[me], self.ssem.at[i], self.rsem.at[i],
                    device_id=(req, t), device_id_type=MESH))
        return out

    def _load(self, n):
        return pltpu.make_async_copy(self.srcs[n].at[lax.axis_index('cp')], self.own.at[n], self.lsem.at[n])

    def _store(self, n):
        return pltpu.make_async_copy(self.own.at[n], self.dsts[n].at[lax.axis_index('cp')], self.lsem.at[n])

    def begin(self):
        if not self.srcs:
            return

        @pl.when(self.first)
        def _():
            me = lax.axis_index('cp')
            req = lax.axis_index('req')
            bar = pltpu.get_barrier_semaphore()
            for o in range(1, self.ncp):
                pl.semaphore_signal(bar, inc=1, device_id=(req, lax.rem(me + o, self.ncp)), device_id_type=MESH)
            pl.semaphore_wait(bar, self.ncp - 1)
            for c in self._remote():
                c.start()
            for n in range(len(self.srcs)):
                self._load(n).start()

    def end(self):
        if not self.srcs:
            return

        @pl.when(self.second)
        def _():
            for n in range(len(self.srcs)):
                self._load(n).wait()
                self._store(n).start()

        @pl.when(self.last)
        def _():
            for n in range(len(self.srcs)):
                self._store(n).wait()
            for c in self._remote():
                c.wait()


def _exchange_scratch(ncp, srcs):
    k = len(srcs)
    if not k:
        return []
    return [pltpu.SemaphoreType.DMA((k * (ncp - 1),)), pltpu.SemaphoreType.DMA((k * (ncp - 1),)),
            pltpu.SemaphoreType.DMA((k,)), pltpu.VMEM((k,) + srcs[0].shape[1:], BF16)]


class _Ids:
    def __init__(self):
        self.n = 0

    def params(self, comm):
        if not comm:
            return pltpu.CompilerParams(vmem_limit_bytes=62 << 20)
        self.n += 1
        return pltpu.CompilerParams(vmem_limit_bytes=62 << 20, collective_id=self.n, has_side_effects=True)


def _only_kernel(ncp, k, *refs):
    srcs, dsts, sc = refs[:k], refs[k:2 * k], refs[2 * k:]
    i = pl.program_id(0)
    ex = _Exchange(ncp, srcs, dsts, sc, i == 0, i == 0, i == 0)
    ex.begin()
    ex.end()


def _only(ids, ncp, srcs):
    k = len(srcs)
    return pl.pallas_call(
        functools.partial(_only_kernel, ncp, k), grid=(1,), in_specs=[HBM] * k, out_specs=[HBM] * k,
        out_shape=[jax.ShapeDtypeStruct(a.shape, a.dtype) for a in srcs],
        scratch_shapes=_exchange_scratch(ncp, srcs), compiler_params=ids.params(True), name='exchange')(*srcs)


def _attn_kernel(high, ncp, seg, big, k, *refs):
    nkv = 4 if high else 2
    q_ref, kv, srcs = refs[0], refs[1:1 + nkv], refs[1 + nkv:1 + nkv + k]
    o_ref, dsts = refs[1 + nkv + k], refs[2 + nkv + k:2 + nkv + 2 * k]
    sc = refs[2 + nkv + 2 * k:]
    m_s, acc, va = sc[0], sc[1], sc[2:2 + nkv // 2]
    b = pl.program_id(0)
    ex = _Exchange(ncp, srcs, dsts, sc[2 + nkv // 2:], b == 0, b == 1, b == ncp - 1) if k else None
    if k:
        ex.begin()
    kh, vh = kv[-2], va[-1]
    rows = kh.shape[0]
    nh = q_ref.shape[1] // HEAD
    scale = HEAD ** -0.5 * LOG2E

    @pl.when(b == 0)
    def _():
        for src, dst in zip(kv[1::2], va):
            for h in range(nh):
                dst[h, :, :HEAD] = src[:, h * HEAD:(h + 1) * HEAD]
                dst[h, :, HEAD:] = jnp.ones((rows, HEAD), BF16)

    m_s[...] = jnp.full_like(m_s, -jnp.inf)
    acc[...] = jnp.zeros_like(acc)

    def chunk(kr, vr, start, size, diag=None):
        start = pl.multiple_of(start, HEAD)
        ss = []
        for h in range(nh):
            hs = slice(h * HEAD, (h + 1) * HEAD)
            s = lax.dot_general(q_ref[:, hs], kr[pl.ds(start, size), hs], (((1,), (1,)), ((), ())),
                                preferred_element_type=F32)
            if diag is not None:
                c = lax.broadcasted_iota(jnp.int32, (seg, size), 1) - diag
                r = lax.broadcasted_iota(jnp.int32, (seg, size), 0)
                ok = c <= r
                if diag == 0 and size > seg:
                    ok = ok | (c >= seg)
                s = jnp.where(ok, s, -jnp.inf)
            ss.append(s)
        for h in range(nh):
            s = ss[h]
            mp = m_s[h]
            mn = jnp.maximum(mp, jnp.max(s, axis=1, keepdims=True))
            mc = mn * scale
            p = jnp.exp2(s * scale - mc[:, :1]).astype(BF16)
            al = jnp.exp2(mp * scale - mc)
            acc[h] = jnp.concatenate([al, al], axis=1) * acc[h] + jnp.dot(
                p, vr[h, pl.ds(start, size)], preferred_element_type=F32)
            m_s[h] = mn

    if high:
        for j in range(rows // big):
            chunk(kv[0], va[0], j * big, big)
    nb = (ncp - 1 - b) if high else b

    def pair(j, _):
        chunk(kh, vh, (rows - (j + 1) * 2 * seg) if high else j * 2 * seg, 2 * seg)
        return 0

    lax.fori_loop(0, nb // 2, pair, 0)

    @pl.when(lax.rem(nb, 2) == 1)
    def _():
        if high:
            chunk(kh, vh, b * seg, 2 * seg, 0)
        else:
            chunk(kh, vh, (b - 1) * seg, 2 * seg, seg)

    @pl.when(lax.rem(nb, 2) == 0)
    def _():
        chunk(kh, vh, b * seg, seg, 0)

    for h in range(nh):
        o_ref[:, h * HEAD:(h + 1) * HEAD] = (acc[h, :, :HEAD] / acc[h, :, HEAD:]).astype(BF16)
    if k:
        ex.end()


def _attention(ids, q, kv, send=()):
    ncp, seg, w = q.shape
    high, nh, k = len(kv) == 4, w // HEAD, len(send)
    rows = ncp * seg
    blk = pl.BlockSpec((None, seg, w), lambda i: (i, 0, 0))
    out = pl.pallas_call(
        functools.partial(_attn_kernel, high, ncp, seg, rows // 2, k),
        grid=(ncp,),
        in_specs=[blk] + [pl.BlockSpec((rows, w), lambda i: (0, 0))] * len(kv) + [HBM] * k,
        out_specs=[blk] + [HBM] * k,
        out_shape=[jax.ShapeDtypeStruct(q.shape, BF16)] + [jax.ShapeDtypeStruct(a.shape, BF16) for a in send],
        scratch_shapes=[pltpu.VMEM((nh, seg, HEAD), F32), pltpu.VMEM((nh, seg, 2 * HEAD), F32)]
        + [pltpu.VMEM((nh, rows, 2 * HEAD), BF16)] * (len(kv) // 2) + _exchange_scratch(ncp, send),
        compiler_params=ids.params(k), name='attn_high' if high else 'attn_low',
    )(q, *[a.reshape(rows, w) for a in kv], *send)
    return out[0], out[1:]


TN = 512


def _norm(x, g):
    x32 = x.astype(F32)
    r = lax.rsqrt(jnp.mean(x32 * x32, axis=-1, keepdims=True) + 1e-5)
    return (x32 * r * g.astype(F32)).astype(BF16)


def _dense_kernel(ncp, nm, nf, nq, cache, k, *refs):
    it = iter(refs)
    take = lambda n: [next(it) for _ in range(n)]
    x_ref, = take(1)
    if nm:
        o_ref, wo, g2, w1, w3, w2 = take(6)
    if nq:
        g1, cos, sin, wq, wk, wv = take(6)
    if cache:
        other, = take(1)
        land = take(8)
    srcs = take(k)
    if nm:
        y_ref, = take(1)
    if nq:
        qo, ko, vo = take(3)
    if cache:
        kc, vc = take(2)
    dsts = take(k)
    h_s, = take(1)
    if nm:
        o_s, x_s, acc = take(3)
    i = pl.program_id(0)
    last = nm + nf + 3 * nq - 1
    if k:
        ex = _Exchange(ncp, srcs, dsts, take(4), i == 0, i == 1, i == last)
        ex.begin()
    if nm:
        @pl.when(i == 0)
        def _():
            w = o_ref.shape[2]
            for j in range(ncp):
                o_s[:, j * w:(j + 1) * w] = o_ref[j]

        for j in range(nm):
            @pl.when(i == j)
            def _():
                ns = slice(j * TN, (j + 1) * TN)
                x_s[:, ns] = (x_ref[:, ns].astype(F32) + jnp.dot(
                    o_s[...], wo[...], preferred_element_type=F32)).astype(BF16)

        @pl.when(i == nm)
        def _():
            h_s[...] = _norm(x_s[...], g2[...])
            acc[...] = jnp.zeros_like(acc)

        @pl.when((i >= nm) & (i < nm + nf))
        def _():
            h = h_s[...]
            a = jnp.dot(h, w1[...], preferred_element_type=F32)
            c = jnp.dot(h, w3[...], preferred_element_type=F32)
            u = (jax.nn.silu(a) * c).astype(BF16)
            acc[...] += jnp.dot(u, w2[...], preferred_element_type=F32)

        @pl.when(i == nm + nf - 1)
        def _():
            y = (x_s[...].astype(F32) + acc[...]).astype(BF16)
            seg = x_s.shape[0]
            if cache:
                y_ref[:seg] = other[...]
                y_ref[seg:] = y
            else:
                y_ref[...] = y
            if nq:
                x_s[...] = y
    if nq:
        s = i - (nm + nf)

        @pl.when(s == 0)
        def _():
            h_s[...] = _norm(x_s[...] if nm else x_ref[...], g1[...])

        def project(w, out, rope):
            t = jnp.dot(h_s[...], w[...], preferred_element_type=F32)
            wd = out.shape[2]
            for j in range(TN // HEAD):
                th = t[:, j * HEAD:(j + 1) * HEAD]
                if rope:
                    th = th * cos[...] + pltpu.roll(th, HEAD // 2, 1) * sin[...]
                lo = j * HEAD % wd
                out[j * HEAD // wd, :, lo:lo + HEAD] = th.astype(BF16)

        @pl.when((s >= 0) & (s < nq))
        def _():
            project(wv, vo, False)

        @pl.when((s >= nq) & (s < 2 * nq))
        def _():
            project(wk, ko, True)

        @pl.when(s >= 2 * nq)
        def _():
            project(wq, qo, True)
    if cache:
        s = i - nm
        half = cache // 2

        def put(out, l, src):
            for h in range(out.shape[2]):
                out[l, :, h, :] = src[:, h * HEAD:(h + 1) * HEAD]

        @pl.when((s >= 0) & (s < half))
        def _():
            for l in range(2):
                put(kc, l, land[l])
                put(vc, l, land[4 + l])

        @pl.when((s >= half) & (s < cache))
        def _():
            for l in range(2):
                put(kc, l, land[2 + l])
                put(vc, l, land[6 + l])
    if k:
        ex.end()


def _dense(ids, ncp, x, half, mlp=None, qkv=None, cache=None, send=()):
    d = x.shape[1]
    seg = x.shape[0] // 2 if half is not None else x.shape[0]
    hb = half or 0
    k = len(send)
    nm = nf = nq = 0
    clamp = lambda v, n: jnp.clip(v, 0, n - 1)
    xs = pl.BlockSpec((seg, d), lambda i: (hb, 0))
    args, specs, outs, ospecs, scratch = [x], [xs], [], [], [pltpu.VMEM((seg, d), BF16)]
    if mlp is not None:
        l, o, wo, g2, w1, w3, w2 = mlp
        ff = w1.shape[2]
        nm, nf = d // TN, ff // TN
        nm_, nf_ = nm, nf
        args += [o, wo, g2, w1, w3, w2]
        specs += [pl.BlockSpec(o.shape, lambda i: (0, 0, 0)),
                  pl.BlockSpec((None, d, TN), lambda i: (l, 0, clamp(i, nm_))),
                  pl.BlockSpec((1, d), lambda i: (0, 0)),
                  pl.BlockSpec((None, d, TN), lambda i: (l, 0, clamp(i - nm_, nf_))),
                  pl.BlockSpec((None, d, TN), lambda i: (l, 0, clamp(i - nm_, nf_))),
                  pl.BlockSpec((None, TN, d), lambda i: (l, clamp(i - nm_, nf_), 0))]
        scratch += [pltpu.VMEM((seg, d), BF16), pltpu.VMEM((seg, d), BF16), pltpu.VMEM((seg, d), F32)]
    base = nm + nf
    if qkv is not None:
        lq, g1, cos, sin, wq, wk, wv = qkv
        nq = wq.shape[2] // TN
        nq_ = nq
        cs = pl.BlockSpec((seg, HEAD), lambda i: (qkv_half, 0))
        qkv_half = 0
        args += [g1, cos, sin, wq, wk, wv]
        specs += [pl.BlockSpec((1, d), lambda i: (0, 0)), cs, cs]
        specs += [pl.BlockSpec((None, d, TN), lambda i, p=p: (lq, 0, clamp(i - base - p * nq_, nq_))) for p in (2, 1, 0)]
    if cache is not None:
        other, land = cache
        w = land[0].shape[2]
        args += [other] + list(land)
        lo = pl.BlockSpec((None, seg, w), lambda i: (clamp(i - nm_, ncp), 0, 0))
        hi = pl.BlockSpec((None, seg, w), lambda i: (ncp - 1 - clamp(i - nm_ - ncp, ncp), 0, 0))
        specs += [pl.BlockSpec((seg, d), lambda i: (0, 0))] + [lo, lo, hi, hi] * 2
    args += list(send)
    specs += [HBM] * k
    if mlp is not None:
        ys = (2 * seg, d) if cache is not None else (seg, d)
        outs.append(jax.ShapeDtypeStruct(ys, BF16))
        ospecs.append(pl.BlockSpec(ys, lambda i: (0, 0)))
    if qkv is not None:
        wd = wq.shape[2] // ncp
        for p in (2, 1, 0):
            outs.append(jax.ShapeDtypeStruct((ncp, seg, wd), BF16))
            ospecs.append(pl.BlockSpec((TN // wd, seg, wd), lambda i, p=p: (clamp(i - base - p * nq_, nq_), 0, 0)))
    if cache is not None:
        for _ in range(2):
            outs.append(jax.ShapeDtypeStruct((2, 2 * ncp * seg, w // HEAD, HEAD), BF16))
            ospecs.append(pl.BlockSpec((2, seg, w // HEAD, HEAD), lambda i: (0, clamp(i - nm_, 2 * ncp), 0, 0)))
    outs += [jax.ShapeDtypeStruct(a.shape, BF16) for a in send]
    ospecs += [HBM] * k
    out = pl.pallas_call(
        functools.partial(_dense_kernel, ncp, nm, nf, nq, 2 * ncp if cache is not None else 0, k),
        grid=(nm + nf + 3 * nq,), in_specs=specs, out_specs=ospecs, out_shape=outs,
        scratch_shapes=scratch + _exchange_scratch(ncp, send), compiler_params=ids.params(k),
        name='dense' + ('_mlp' if nm else '') + ('_qkv' if nq else ''))(*args)
    return out[:len(out) - k], out[len(out) - k:]


def _angles(pos):
    half = HEAD // 2
    inv = 1.0 / (10000.0 ** (jnp.arange(half, dtype=F32) * (2.0 / HEAD)))
    ang = pos.astype(F32)[:, None] * inv
    c, s = jnp.cos(ang), jnp.sin(ang)
    return jnp.concatenate([c, c], axis=-1), jnp.concatenate([-s, s], axis=-1)


def solution(mesh):
    ncp = mesh.shape['cp']
    act = P(('req', 'cp'), None)
    cache = P(None, 'req', 'cp', None)

    def body(x, pos, g1, g2, wq, wk, wv, wo, w1, w3, w2):
        ids = _Ids()
        seg = x.shape[0] // 2
        cos, sin = _angles(pos)
        cl, sl, ch, sh = cos[:seg], sin[:seg], cos[seg:], sin[seg:]

        def qkv(l, c, s):
            return (l, g1[l:l + 1], c, s, wq, wk, wv)

        def mlp(l, o):
            return (l, o, wo, g2[l:l + 1], w1, w3, w2)

        dense = functools.partial(_dense, ids, ncp)
        a0l, _ = dense(x, 0, qkv=qkv(0, cl, sl))
        a0h, (q, k0l, v0l) = dense(x, 1, qkv=qkv(0, ch, sh), send=a0l)
        o, (v0h,) = _attention(ids, q, (k0l, v0l), send=(a0h[2],))
        (o,) = _only(ids, ncp, (o,))
        (xl, *a1l), (qh, k0h) = dense(x, 0, mlp=mlp(0, o), qkv=qkv(1, cl, sl), send=(a0h[0], a0h[1]))
        oh, (q, k1l, v1l) = _attention(ids, qh, (k0l, v0l, k0h, v0h), send=tuple(a1l))
        o, (oh,) = _attention(ids, q, (k1l, v1l), send=(oh,))
        (xh, *a1h), (o,) = dense(x, 1, mlp=mlp(0, oh), qkv=qkv(1, ch, sh), send=(o,))
        (xl,), (q, k1h, v1h) = dense(xl, None, mlp=mlp(1, o), send=tuple(a1h))
        o, _ = _attention(ids, q, (k1l, v1l, k1h, v1h))
        (o,) = _only(ids, ncp, (o,))
        (y, kc, vc), _ = dense(xh, None, mlp=mlp(1, o), cache=(xl, (k0l, k1l, k0h, k1h, v0l, v1l, v0h, v1h)))
        return y, kc, vc

    return jax.shard_map(body, mesh=mesh, in_specs=(act, P(('req', 'cp'))) + (P(),) * 9,
                         out_specs=(act, cache, cache), check_vma=False)
```

```python
import functools

import jax
import jax.numpy as jnp
from jax import lax
from jax.experimental import pallas as pl
from jax.experimental.pallas import tpu as pltpu
from jax.sharding import PartitionSpec as P

HEAD = 128
F32 = jnp.float32
BF16 = jnp.bfloat16
LOG2E = 1.4426950408889634
MESH = pl.DeviceIdType.MESH
HBM = pl.BlockSpec(memory_space=pltpu.HBM)


class _Exchange:
    def __init__(self, ncp, srcs, dsts, scratch, first, second, last):
        self.ncp, self.srcs, self.dsts = ncp, srcs, dsts
        self.ssem, self.rsem, self.lsem, self.own = scratch
        self.first, self.second, self.last = first, second, last

    def _remote(self):
        me = lax.axis_index('cp')
        req = lax.axis_index('req')
        out = []
        for n, (s, d) in enumerate(zip(self.srcs, self.dsts)):
            for o in range(1, self.ncp):
                t = lax.rem(me + o, self.ncp)
                i = n * (self.ncp - 1) + o - 1
                out.append(pltpu.make_async_remote_copy(
                    s.at[t], d.at[me], self.ssem.at[i], self.rsem.at[i],
                    device_id=(req, t), device_id_type=MESH))
        return out

    def _load(self, n):
        return pltpu.make_async_copy(self.srcs[n].at[lax.axis_index('cp')], self.own.at[n], self.lsem.at[n])

    def _store(self, n):
        return pltpu.make_async_copy(self.own.at[n], self.dsts[n].at[lax.axis_index('cp')], self.lsem.at[n])

    def begin(self, greet=True):
        @pl.when(self.first)
        def _():
            if greet:
                _greet(self.ncp)
            for c in self._remote():
                c.start()
            for n in range(len(self.srcs)):
                self._load(n).start()

    def end(self):
        @pl.when(self.second)
        def _():
            for n in range(len(self.srcs)):
                self._load(n).wait()
                self._store(n).start()

        @pl.when(self.last)
        def _():
            for n in range(len(self.srcs)):
                self._store(n).wait()
            for c in self._remote():
                c.wait()


def _exchange_scratch(ncp, srcs):
    k = len(srcs)
    if not k:
        return []
    return [pltpu.SemaphoreType.DMA((k * (ncp - 1),)), pltpu.SemaphoreType.DMA((k * (ncp - 1),)),
            pltpu.SemaphoreType.DMA((k,)), pltpu.VMEM((k,) + srcs[0].shape[1:], BF16)]


class _Ids:
    def __init__(self):
        self.n = 0

    def params(self, comm):
        if not comm:
            return pltpu.CompilerParams(vmem_limit_bytes=62 << 20)
        self.n += 1
        return pltpu.CompilerParams(vmem_limit_bytes=62 << 20, collective_id=self.n, has_side_effects=True)


def _greet(ncp):
    me = lax.axis_index('cp')
    req = lax.axis_index('req')
    bar = pltpu.get_barrier_semaphore()
    for o in range(1, ncp):
        pl.semaphore_signal(bar, inc=1, device_id=(req, lax.rem(me + o, ncp)), device_id_type=MESH)
    pl.semaphore_wait(bar, ncp - 1)


EXTRA = 16


def _attn_kernel(high, ncp, k, *refs):
    nkv = 4 if high else 2
    q_ref, kv, srcs = refs[0], refs[1:1 + nkv], refs[1 + nkv:1 + nkv + k]
    land, dsts = refs[1 + nkv + k], refs[2 + nkv + k:2 + nkv + 2 * k]
    sc = refs[2 + nkv + 2 * k:]
    s_s, m_s, acc, out, ssem, rsem, lsem = sc[:7]
    vt = sc[7:7 + nkv // 2]
    i = pl.program_id(0)
    rows, w = q_ref.shape
    seg = rows // ncp
    c2 = 2 * seg
    npair = ncp // 2
    nh = w // HEAD
    scale = HEAD ** -0.5 * LOG2E
    me = lax.axis_index('cp')
    req = lax.axis_index('req')
    b = lax.rem(me // 2 + 1 + i, npair)
    ex = _Exchange(ncp, srcs, dsts, sc[7 + nkv // 2:], i == 0, i == 1, i == npair - 1) if k else None

    @pl.when(i == 0)
    def _():
        _greet(ncp)

    if k:
        ex.begin(greet=False)

    @pl.when(i == 0)
    def _():
        for src, dst in zip(kv[1::2], vt):
            for h in range(nh):
                for j in range(npair):
                    dst[h, :HEAD, j * c2:(j + 1) * c2] = src[j * c2:(j + 1) * c2, h * HEAD:(h + 1) * HEAD].T
                dst[h, HEAD:, :] = jnp.ones((EXTRA, rows), BF16)

    m_s[...] = jnp.full_like(m_s, -jnp.inf)
    acc[...] = jnp.zeros_like(acc)

    def scores(kr, start, h):
        hs = slice(h * HEAD, (h + 1) * HEAD)
        s_s[h] = lax.dot_general(kr[pl.ds(pl.multiple_of(start, c2), c2), hs], q_ref[pl.ds(pl.multiple_of(b * c2, c2), c2), hs],
                                 (((1,), (1,)), ((), ())), preferred_element_type=F32)

    def update(vr, start, h, mask=False):
        s = s_s[h]
        if mask:
            r = lax.broadcasted_iota(jnp.int32, (c2, c2), 0)
            c = lax.broadcasted_iota(jnp.int32, (c2, c2), 1)
            if high:
                r = jnp.where(r >= seg, r - seg, r + seg)
                c = jnp.where(c >= seg, c - seg, c + seg)
            s = jnp.where(r <= c, s, -jnp.inf)
        mp = m_s[h]
        mn = jnp.maximum(mp, jnp.max(s, axis=0, keepdims=True))
        mc = mn * scale
        p = jnp.exp2(s * scale - mc).astype(BF16)
        al = jnp.exp2(mp * scale - mc)
        acc[h] = acc[h] * al + jnp.dot(vr[h, :, pl.ds(pl.multiple_of(start, c2), c2)], p, preferred_element_type=F32)
        m_s[h] = mn

    def chunk(kr, vr, start, nkr, nstart):
        for h in range(nh):
            if h + 1 < nh:
                scores(kr, start, h + 1)
            else:
                scores(nkr, nstart, 0)
            update(vr, start, h)

    kh, vh = kv[-2], vt[-1]
    nb = (npair - 1 - b) if high else b

    def at(j):
        return (npair - 1 - j) * c2 if high else j * c2

    if high:
        scores(kv[0], 0, 0)
        for j in range(npair):
            if j + 1 < npair:
                chunk(kv[0], vt[0], j * c2, kv[0], (j + 1) * c2)
            else:
                chunk(kv[0], vt[0], j * c2, kh, at(0))
    else:
        scores(kh, 0, 0)

    def body(j, _):
        chunk(kh, vh, at(j), kh, at(j + 1))
        return 0

    lax.fori_loop(0, nb, body, 0)
    for h in range(nh):
        if h + 1 < nh:
            scores(kh, b * c2, h + 1)
        update(vh, b * c2, h, True)
    for h in range(nh):
        o = acc[h, :HEAD] / acc[h, HEAD:HEAD + 1]
        out[i, :, h * HEAD:(h + 1) * HEAD] = o.T.astype(BF16)

    def send(step, pair, e):
        return pltpu.make_async_remote_copy(
            out.at[step, pl.ds(e * seg, seg)], land.at[me], ssem.at[2 * step + e], rsem.at[2 * step + lax.rem(me, 2)],
            device_id=(req, 2 * pair + e), device_id_type=MESH)

    @pl.when(i < npair - 1)
    def _():
        for e in range(2):
            send(i, b, e).start()

    @pl.when(i == npair - 1)
    def _():
        mine = lax.rem(me, 2)
        peer = 1 - mine
        last = npair - 1
        own = pltpu.make_async_copy(out.at[last, pl.ds(mine * seg, seg)], land.at[me], lsem)
        own.start()
        twin = pltpu.make_async_remote_copy(
            out.at[last, pl.ds(peer * seg, seg)], land.at[me], ssem.at[2 * last], rsem.at[2 * last],
            device_id=(req, me + 1 - 2 * mine), device_id_type=MESH)
        twin.start()
        for step in range(last):
            pair = lax.rem(me // 2 + 1 + step, npair)
            for e in range(2):
                send(step, pair, e).wait_send()
                src = 2 * lax.rem(me // 2 + npair - 1 - step, npair) + e
                pltpu.make_async_remote_copy(
                    out.at[step, pl.ds(e * seg, seg)], land.at[src], ssem.at[2 * step + e], rsem.at[2 * step + e],
                    device_id=(req, src), device_id_type=MESH).wait_recv()
        twin.wait()
        own.wait()

    if k:
        ex.end()


def _attention(ids, q, kv, send=()):
    ncp, seg, w = q.shape
    high, nh, k = len(kv) == 4, w // HEAD, len(send)
    rows, c2, npair = ncp * seg, 2 * seg, ncp // 2
    flat = pl.BlockSpec((rows, w), lambda i: (0, 0))
    out = pl.pallas_call(
        functools.partial(_attn_kernel, high, ncp, k),
        grid=(npair,),
        in_specs=[flat] * (1 + len(kv)) + [HBM] * k,
        out_specs=[HBM] * (1 + k),
        out_shape=[jax.ShapeDtypeStruct(a.shape, BF16) for a in (q,) + tuple(send)],
        scratch_shapes=[pltpu.VMEM((nh, c2, c2), F32), pltpu.VMEM((nh, 1, c2), F32), pltpu.VMEM((nh, HEAD + EXTRA, c2), F32),
                        pltpu.VMEM((npair, c2, w), BF16), pltpu.SemaphoreType.DMA((ncp,)), pltpu.SemaphoreType.DMA((ncp,)),
                        pltpu.SemaphoreType.DMA]
        + [pltpu.VMEM((nh, HEAD + EXTRA, rows), BF16)] * (len(kv) // 2) + _exchange_scratch(ncp, send),
        compiler_params=ids.params(True), name='attn_high' if high else 'attn_low',
    )(q.reshape(rows, w), *[a.reshape(rows, w) for a in kv], *send)
    return out[0], out[1:]


def _first_kernel(ncp, nq, x_ref, g1, cos, sin, wq, wk, wv, qh, kh, vh, ql, kl, vl, h_s, buf, ssem, rsem, lsem):
    i = pl.program_id(0)
    me = lax.axis_index('cp')
    req = lax.axis_index('req')
    seg = x_ref.shape[0] // 2
    wd = qh.shape[2]
    per = TN // wd

    @pl.when(i == 0)
    def _():
        _greet(ncp)
        h_s[...] = _norm(x_ref[...], g1[0:1])

    def remote(p, t, dst):
        return pltpu.make_async_remote_copy(buf.at[p, t], dst.at[me], ssem.at[p * ncp + t], rsem.at[p * ncp + me],
                                            device_id=(req, t), device_id_type=MESH)

    def own(p, dst):
        return pltpu.make_async_copy(buf.at[p, me], dst.at[me], lsem.at[p])

    def project(p, w, high, low, rope):
        n = i - p * nq
        t = jnp.dot(h_s[...], w[...], preferred_element_type=F32)
        for j in range(TN // HEAD):
            th = t[:, j * HEAD:(j + 1) * HEAD]
            if rope:
                th = th * cos[...] + pltpu.roll(th, HEAD // 2, 1) * sin[...]
            th = th.astype(BF16)
            lo = j * HEAD % wd
            e = j * HEAD // wd
            buf[p, per * n + e, :, lo:lo + HEAD] = th[:seg]
            high[e, :, lo:lo + HEAD] = th[seg:]
        for e in range(per):
            to = per * n + e

            @pl.when(to != me)
            def _():
                remote(p, to, low).start()

            @pl.when(to == me)
            def _():
                own(p, low).start()

    @pl.when(i < nq)
    def _():
        project(0, wv, vh, vl, False)

    @pl.when((i >= nq) & (i < 2 * nq))
    def _():
        project(1, wk, kh, kl, True)

    @pl.when(i >= 2 * nq)
    def _():
        project(2, wq, qh, ql, True)

    @pl.when(i == 3 * nq - 1)
    def _():
        for p, dst in enumerate((vl, kl, ql)):
            own(p, dst).wait()
            for o in range(1, ncp):
                t = lax.rem(me + o, ncp)
                remote(p, t, dst).wait_send()
                pltpu.make_async_remote_copy(buf.at[p, t], dst.at[t], ssem.at[p * ncp + t], rsem.at[p * ncp + t],
                                             device_id=(req, t), device_id_type=MESH).wait_recv()


def _first(ids, ncp, x, g1, cos, sin, wq, wk, wv):
    rows, d = x.shape
    seg, wd, nq = rows // 2, wq.shape[2] // ncp, wq.shape[2] // TN
    clamp = lambda v, n: jnp.clip(v, 0, n - 1)
    full = lambda a: pl.BlockSpec(a.shape, lambda i: (0, 0))
    blocks = jax.ShapeDtypeStruct((ncp, seg, wd), BF16)
    out = pl.pallas_call(
        functools.partial(_first_kernel, ncp, nq), grid=(3 * nq,),
        in_specs=[full(x), full(g1), full(cos), full(sin)]
        + [pl.BlockSpec((None, d, TN), lambda i, p=p: (0, 0, clamp(i - p * nq, nq))) for p in (2, 1, 0)],
        out_specs=[pl.BlockSpec((TN // wd, seg, wd), lambda i, p=p: (clamp(i - p * nq, nq), 0, 0)) for p in (2, 1, 0)] + [HBM] * 3,
        out_shape=[blocks] * 6,
        scratch_shapes=[pltpu.VMEM((rows, d), BF16), pltpu.VMEM((3, ncp, seg, wd), BF16), pltpu.SemaphoreType.DMA((3 * ncp,)),
                        pltpu.SemaphoreType.DMA((3 * ncp,)), pltpu.SemaphoreType.DMA((3,))],
        compiler_params=ids.params(True), name='first_qkv')(x, g1, cos, sin, wq, wk, wv)
    return out[:3], out[3:]


TN = 512


def _norm(x, g):
    x32 = x.astype(F32)
    r = lax.rsqrt(jnp.mean(x32 * x32, axis=-1, keepdims=True) + 1e-5)
    return (x32 * r * g.astype(F32)).astype(BF16)


def _dense_kernel(ncp, nm, nf, nq, lm, lq, cache, k, *refs):
    it = iter(refs)
    take = lambda n: [next(it) for _ in range(n)]
    x_ref, = take(1)
    if nm:
        o_ref, wo, g2, w1, w3, w2 = take(6)
    if nq:
        g1, cos, sin, wq, wk, wv = take(6)
    if cache:
        other, = take(1)
        land = take(8)
    srcs = take(k)
    if nm:
        y_ref, = take(1)
    if nq:
        qo, ko, vo = take(3)
    if cache:
        kc, vc = take(2)
    dsts = take(k)
    h_s, = take(1)
    if nm:
        o_s, x_s, acc = take(3)
    i = pl.program_id(0)
    last = nm + nf + 3 * nq - 1
    if k:
        ex = _Exchange(ncp, srcs, dsts, take(4), i == 0, i == 1, i == last)
        ex.begin()
    if nm:
        @pl.when(i == 0)
        def _():
            w = o_ref.shape[2]
            for j in range(ncp):
                o_s[:, j * w:(j + 1) * w] = o_ref[j]

        for j in range(nm):
            @pl.when(i == j)
            def _():
                ns = slice(j * TN, (j + 1) * TN)
                x_s[:, ns] = (x_ref[:, ns].astype(F32) + jnp.dot(
                    o_s[...], wo[...], preferred_element_type=F32)).astype(BF16)

        @pl.when(i == nm)
        def _():
            h_s[...] = _norm(x_s[...], g2[lm:lm + 1])
            acc[...] = jnp.zeros_like(acc)

        @pl.when((i >= nm) & (i < nm + nf))
        def _():
            h = h_s[...]
            a = jnp.dot(h, w1[...], preferred_element_type=F32)
            c = jnp.dot(h, w3[...], preferred_element_type=F32)
            u = (jax.nn.silu(a) * c).astype(BF16)
            acc[...] += jnp.dot(u, w2[...], preferred_element_type=F32)

        @pl.when(i == nm + nf - 1)
        def _():
            y = (x_s[...].astype(F32) + acc[...]).astype(BF16)
            seg = x_s.shape[0]
            if cache:
                y_ref[:seg] = other[...]
                y_ref[seg:] = y
            else:
                y_ref[...] = y
            if nq:
                x_s[...] = y
    if nq:
        s = i - (nm + nf)

        @pl.when(s == 0)
        def _():
            h_s[...] = _norm(x_s[...], g1[lq:lq + 1])

        def project(w, out, rope):
            t = jnp.dot(h_s[...], w[...], preferred_element_type=F32)
            wd = out.shape[2]
            for j in range(TN // HEAD):
                th = t[:, j * HEAD:(j + 1) * HEAD]
                if rope:
                    th = th * cos[...] + pltpu.roll(th, HEAD // 2, 1) * sin[...]
                lo = j * HEAD % wd
                out[j * HEAD // wd, :, lo:lo + HEAD] = th.astype(BF16)

        @pl.when((s >= 0) & (s < nq))
        def _():
            project(wv, vo, False)

        @pl.when((s >= nq) & (s < 2 * nq))
        def _():
            project(wk, ko, True)

        @pl.when(s >= 2 * nq)
        def _():
            project(wq, qo, True)
    if cache:
        s = i - nm
        half = cache // 2

        def put(out, l, src):
            out[l] = src[...].reshape(out.shape[1:])

        @pl.when((s >= 0) & (s < half))
        def _():
            for l in range(2):
                put(kc, l, land[l])
                put(vc, l, land[4 + l])

        @pl.when((s >= half) & (s < cache))
        def _():
            for l in range(2):
                put(kc, l, land[2 + l])
                put(vc, l, land[6 + l])
    if k:
        ex.end()


def _dense(ids, ncp, x, half, mlp=None, qkv=None, cache=None, send=()):
    d = x.shape[1]
    seg = x.shape[0] // 2 if half is not None else x.shape[0]
    hb = half or 0
    k = len(send)
    nm = nf = nq = l = lq = 0
    clamp = lambda v, n: jnp.clip(v, 0, n - 1)
    xs = pl.BlockSpec((seg, d), lambda i: (hb, 0))
    args, specs, outs, ospecs, scratch = [x], [xs], [], [], [pltpu.VMEM((seg, d), BF16)]
    if mlp is not None:
        l, o, wo, g2, w1, w3, w2 = mlp
        ff = w1.shape[2]
        nm, nf = d // TN, ff // TN
        nm_, nf_ = nm, nf
        args += [o, wo, g2, w1, w3, w2]
        specs += [pl.BlockSpec(o.shape, lambda i: (0, 0, 0)),
                  pl.BlockSpec((None, d, TN), lambda i: (l, 0, clamp(i, nm_))),
                  pl.BlockSpec(g2.shape, lambda i: (0, 0)),
                  pl.BlockSpec((None, d, TN), lambda i: (l, 0, clamp(i - nm_, nf_))),
                  pl.BlockSpec((None, d, TN), lambda i: (l, 0, clamp(i - nm_, nf_))),
                  pl.BlockSpec((None, TN, d), lambda i: (l, clamp(i - nm_, nf_), 0))]
        scratch += [pltpu.VMEM((seg, d), BF16), pltpu.VMEM((seg, d), BF16), pltpu.VMEM((seg, d), F32)]
    base = nm + nf
    if qkv is not None:
        lq, g1, cos, sin, wq, wk, wv = qkv
        nq = wq.shape[2] // TN
        nq_ = nq
        cs = pl.BlockSpec((seg, HEAD), lambda i: (hb, 0))
        args += [g1, cos, sin, wq, wk, wv]
        specs += [pl.BlockSpec(g1.shape, lambda i: (0, 0)), cs, cs]
        specs += [pl.BlockSpec((None, d, TN), lambda i, p=p: (lq, 0, clamp(i - base - p * nq_, nq_))) for p in (2, 1, 0)]
    if cache is not None:
        other, land = cache
        w = land[0].shape[2]
        args += [other] + list(land)
        lo = pl.BlockSpec((None, seg, w), lambda i: (clamp(i - nm_, ncp), 0, 0))
        hi = pl.BlockSpec((None, seg, w), lambda i: (ncp - 1 - clamp(i - nm_ - ncp, ncp), 0, 0))
        specs += [pl.BlockSpec((seg, d), lambda i: (0, 0))] + [lo, lo, hi, hi] * 2
    args += list(send)
    specs += [HBM] * k
    if mlp is not None:
        ys = (2 * seg, d) if cache is not None else (seg, d)
        outs.append(jax.ShapeDtypeStruct(ys, BF16))
        ospecs.append(pl.BlockSpec(ys, lambda i: (0, 0)))
    if qkv is not None:
        wd = wq.shape[2] // ncp
        for p in (2, 1, 0):
            outs.append(jax.ShapeDtypeStruct((ncp, seg, wd), BF16))
            ospecs.append(pl.BlockSpec((TN // wd, seg, wd), lambda i, p=p: (clamp(i - base - p * nq_, nq_), 0, 0)))
    if cache is not None:
        for _ in range(2):
            outs.append(jax.ShapeDtypeStruct((2, 2 * ncp * seg, w // HEAD, HEAD), BF16))
            ospecs.append(pl.BlockSpec((2, seg, w // HEAD, HEAD), lambda i: (0, clamp(i - nm_, 2 * ncp), 0, 0)))
    outs += [jax.ShapeDtypeStruct(a.shape, BF16) for a in send]
    ospecs += [HBM] * k
    out = pl.pallas_call(
        functools.partial(_dense_kernel, ncp, nm, nf, nq, l, lq, 2 * ncp if cache is not None else 0, k),
        grid=(nm + nf + 3 * nq,), in_specs=specs, out_specs=ospecs, out_shape=outs,
        scratch_shapes=scratch + _exchange_scratch(ncp, send), compiler_params=ids.params(k),
        name='dense' + ('_mlp' if nm else '') + ('_qkv' if nq else ''))(*args)
    return out[:len(out) - k], out[len(out) - k:]


def _angles(pos):
    half = HEAD // 2
    inv = 1.0 / (10000.0 ** (jnp.arange(half, dtype=F32) * (2.0 / HEAD)))
    ang = pos.astype(F32)[:, None] * inv
    c, s = jnp.cos(ang), jnp.sin(ang)
    return jnp.concatenate([c, c], axis=-1), jnp.concatenate([-s, s], axis=-1)


def solution(mesh):
    ncp = mesh.shape['cp']
    act = P(('req', 'cp'), None)
    cache = P(None, 'req', 'cp', None)

    def body(x, pos, g1, g2, wq, wk, wv, wo, w1, w3, w2):
        ids = _Ids()
        cos, sin = _angles(pos)

        def mlp(l, o):
            return (l, o, wo, g2, w1, w3, w2)

        qkv = (1, g1, cos, sin, wq, wk, wv)
        dense = functools.partial(_dense, ids, ncp)
        a0h, (q, k0l, v0l) = _first(ids, ncp, x, g1, cos, sin, wq, wk, wv)
        o, _ = _attention(ids, q, (k0l, v0l))
        (xl, *a1l), (q, k0h, v0h) = dense(x, 0, mlp=mlp(0, o), qkv=qkv, send=tuple(a0h))
        o, (v1l,) = _attention(ids, q, (k0l, v0l, k0h, v0h), send=(a1l[2],))
        (xh, *a1h), (q, k1l) = dense(x, 1, mlp=mlp(0, o), qkv=qkv, send=(a1l[0], a1l[1]))
        o, _ = _attention(ids, q, (k1l, v1l))
        (xl,), (q, k1h, v1h) = dense(xl, None, mlp=mlp(1, o), send=tuple(a1h))
        o, _ = _attention(ids, q, (k1l, v1l, k1h, v1h))
        (y, kc, vc), _ = dense(xh, None, mlp=mlp(1, o), cache=(xl, (k0l, k1l, k0h, k1h, v0l, v1l, v0h, v1h)))
        return y, kc, vc

    return jax.shard_map(body, mesh=mesh, in_specs=(act, P(('req', 'cp'))) + (P(),) * 9,
                         out_specs=(act, cache, cache), check_vma=False)
```

```python
import functools

import jax
import jax.numpy as jnp
from jax import lax
from jax.experimental import pallas as pl
from jax.experimental.pallas import tpu as pltpu
from jax.sharding import PartitionSpec as P

HEAD = 128
F32 = jnp.float32
BF16 = jnp.bfloat16
LOG2E = 1.4426950408889634
MESH = pl.DeviceIdType.MESH
HBM = pl.BlockSpec(memory_space=pltpu.HBM)


class _Exchange:
    def __init__(self, ncp, srcs, dsts, scratch, first, second, last):
        self.ncp, self.srcs, self.dsts = ncp, srcs, dsts
        self.ssem, self.rsem, self.lsem, self.own = scratch
        self.first, self.second, self.last = first, second, last

    def _remote(self):
        me = lax.axis_index('cp')
        req = lax.axis_index('req')
        out = []
        for n, (s, d) in enumerate(zip(self.srcs, self.dsts)):
            for o in range(1, self.ncp):
                t = lax.rem(me + o, self.ncp)
                i = n * (self.ncp - 1) + o - 1
                out.append(pltpu.make_async_remote_copy(
                    s.at[t], d.at[me], self.ssem.at[i], self.rsem.at[i],
                    device_id=(req, t), device_id_type=MESH))
        return out

    def _load(self, n):
        return pltpu.make_async_copy(self.srcs[n].at[lax.axis_index('cp')], self.own.at[n], self.lsem.at[n])

    def _store(self, n):
        return pltpu.make_async_copy(self.own.at[n], self.dsts[n].at[lax.axis_index('cp')], self.lsem.at[n])

    def begin(self, greet=True):
        @pl.when(self.first)
        def _():
            if greet:
                _greet(self.ncp)
            for c in self._remote():
                c.start()
            for n in range(len(self.srcs)):
                self._load(n).start()

    def end(self):
        @pl.when(self.second)
        def _():
            for n in range(len(self.srcs)):
                self._load(n).wait()
                self._store(n).start()

        @pl.when(self.last)
        def _():
            for n in range(len(self.srcs)):
                self._store(n).wait()
            for c in self._remote():
                c.wait()


def _exchange_scratch(ncp, srcs):
    k = len(srcs)
    if not k:
        return []
    return [pltpu.SemaphoreType.DMA((k * (ncp - 1),)), pltpu.SemaphoreType.DMA((k * (ncp - 1),)),
            pltpu.SemaphoreType.DMA((k,)), pltpu.VMEM((k,) + srcs[0].shape[1:], BF16)]


class _Ids:
    def __init__(self):
        self.n = 0

    def params(self, comm):
        if not comm:
            return pltpu.CompilerParams(vmem_limit_bytes=62 << 20)
        self.n += 1
        return pltpu.CompilerParams(vmem_limit_bytes=62 << 20, collective_id=self.n, has_side_effects=True)


def _greet(ncp):
    me = lax.axis_index('cp')
    req = lax.axis_index('req')
    bar = pltpu.get_barrier_semaphore()
    for o in range(1, ncp):
        pl.semaphore_signal(bar, inc=1, device_id=(req, lax.rem(me + o, ncp)), device_id_type=MESH)
    pl.semaphore_wait(bar, ncp - 1)


EXTRA = 16


def _attn_kernel(high, ncp, nq, lq, k, *refs):
    nkv = 4 if high else 2
    it = iter(refs)
    take = lambda n: [next(it) for _ in range(n)]
    q_ref, = take(1)
    kv = take(nkv)
    if nq:
        x_ref, g1, cos, sin, wq, wk, wv = take(7)
    srcs = take(k)
    land, = take(1)
    if nq:
        qkv_out = take(3)
    dsts = take(k)
    if nq:
        h_s, = take(1)
    sc = list(it)
    s_s, m_s, acc, out, ssem, rsem, lsem = sc[:7]
    vt = sc[7:7 + nkv // 2]
    i = pl.program_id(0)
    rows, w = q_ref.shape
    seg = rows // ncp
    c2 = 2 * seg
    npair = ncp // 2
    nh = w // HEAD
    final = npair + 3 * nq - 1
    scale = HEAD ** -0.5 * LOG2E
    me = lax.axis_index('cp')
    req = lax.axis_index('req')
    b = lax.rem(me // 2 + 1 + i, npair)
    ex = _Exchange(ncp, srcs, dsts, sc[7 + nkv // 2:], i == 0, i == 1, i == final) if k else None

    @pl.when(i == 0)
    def _():
        _greet(ncp)

    if k:
        ex.begin(greet=False)

    @pl.when(i == 0)
    def _():
        for src, dst in zip(kv[1::2], vt):
            for h in range(nh):
                for j in range(npair):
                    dst[h, :HEAD, j * c2:(j + 1) * c2] = src[j * c2:(j + 1) * c2, h * HEAD:(h + 1) * HEAD].T
                dst[h, HEAD:, :] = jnp.ones((EXTRA, rows), BF16)

    def scores(kr, start, h):
        hs = slice(h * HEAD, (h + 1) * HEAD)
        s_s[h] = lax.dot_general(kr[pl.ds(pl.multiple_of(start, c2), c2), hs], q_ref[pl.ds(pl.multiple_of(b * c2, c2), c2), hs],
                                 (((1,), (1,)), ((), ())), preferred_element_type=F32)

    def update(vr, start, h, mask=False):
        s = s_s[h]
        if mask:
            r = lax.broadcasted_iota(jnp.int32, (c2, c2), 0)
            c = lax.broadcasted_iota(jnp.int32, (c2, c2), 1)
            if high:
                r = jnp.where(r >= seg, r - seg, r + seg)
                c = jnp.where(c >= seg, c - seg, c + seg)
            s = jnp.where(r <= c, s, -jnp.inf)
        mp = m_s[h]
        mn = jnp.maximum(mp, jnp.max(s, axis=0, keepdims=True))
        mc = mn * scale
        p = jnp.exp2(s * scale - mc).astype(BF16)
        al = jnp.exp2(mp * scale - mc)
        acc[h] = acc[h] * al + jnp.dot(vr[h, :, pl.ds(pl.multiple_of(start, c2), c2)], p, preferred_element_type=F32)
        m_s[h] = mn

    def chunk(kr, vr, start, nkr, nstart):
        for h in range(nh):
            if h + 1 < nh:
                scores(kr, start, h + 1)
            else:
                scores(nkr, nstart, 0)
            update(vr, start, h)

    kh, vh = kv[-2], vt[-1]
    nb = (npair - 1 - b) if high else b

    def at(j):
        return (npair - 1 - j) * c2 if high else j * c2

    def attend():
        m_s[...] = jnp.full_like(m_s, -jnp.inf)
        acc[...] = jnp.zeros_like(acc)
        if high:
            scores(kv[0], 0, 0)
            for j in range(npair):
                if j + 1 < npair:
                    chunk(kv[0], vt[0], j * c2, kv[0], (j + 1) * c2)
                else:
                    chunk(kv[0], vt[0], j * c2, kh, at(0))
        else:
            scores(kh, 0, 0)

        def body(j, _):
            chunk(kh, vh, at(j), kh, at(j + 1))
            return 0

        lax.fori_loop(0, nb, body, 0)
        for h in range(nh):
            if h + 1 < nh:
                scores(kh, b * c2, h + 1)
            update(vh, b * c2, h, True)
        for h in range(nh):
            o = acc[h, :HEAD] / acc[h, HEAD:HEAD + 1]
            out[i, :, h * HEAD:(h + 1) * HEAD] = o.T.astype(BF16)

    if nq:
        pl.when(i < npair)(attend)
    else:
        attend()

    def send(step, pair, e):
        return pltpu.make_async_remote_copy(
            out.at[step, pl.ds(e * seg, seg)], land.at[me], ssem.at[2 * step + e], rsem.at[2 * step + lax.rem(me, 2)],
            device_id=(req, 2 * pair + e), device_id_type=MESH)

    @pl.when(i < npair - 1)
    def _():
        for e in range(2):
            send(i, b, e).start()

    mine = lax.rem(me, 2)
    last = npair - 1
    own = pltpu.make_async_copy(out.at[last, pl.ds(mine * seg, seg)], land.at[me], lsem)
    twin = pltpu.make_async_remote_copy(
        out.at[last, pl.ds((1 - mine) * seg, seg)], land.at[me], ssem.at[2 * last], rsem.at[2 * last],
        device_id=(req, me + 1 - 2 * mine), device_id_type=MESH)

    @pl.when(i == last)
    def _():
        own.start()
        twin.start()

    if nq:
        @pl.when(i == npair)
        def _():
            h_s[...] = _norm(x_ref[...], g1[lq:lq + 1])

        _project(i - npair, nq, h_s, (wq, wk, wv), cos, sin, qkv_out)

    @pl.when(i == final)
    def _():
        for step in range(last):
            pair = lax.rem(me // 2 + 1 + step, npair)
            for e in range(2):
                send(step, pair, e).wait_send()
                src = 2 * lax.rem(me // 2 + npair - 1 - step, npair) + e
                pltpu.make_async_remote_copy(
                    out.at[step, pl.ds(e * seg, seg)], land.at[src], ssem.at[2 * step + e], rsem.at[2 * step + e],
                    device_id=(req, src), device_id_type=MESH).wait_recv()
        twin.wait()
        own.wait()

    if k:
        ex.end()


def _attention(ids, q, kv, send=(), qkv=None):
    ncp, seg, w = q.shape
    high, nh, k = len(kv) == 4, w // HEAD, len(send)
    rows, c2, npair = ncp * seg, 2 * seg, ncp // 2
    flat = pl.BlockSpec((rows, w), lambda i: (0, 0), pipeline_mode=pl.Buffered(1))
    args, specs = [q.reshape(rows, w)] + [a.reshape(rows, w) for a in kv], [flat] * (1 + len(kv))
    outs, ospecs, scratch, nq, lq = [jax.ShapeDtypeStruct(q.shape, BF16)], [HBM], [], 0, 0
    if qkv is not None:
        x, half, lq, g1, cos, sin, wq, wk, wv = qkv
        d = x.shape[1]
        nq = wq.shape[2] // TQ
        clamp = lambda v, n: jnp.clip(v, 0, n - 1)
        cs = pl.BlockSpec((seg, HEAD), lambda i: (half, 0))
        args += [x, g1, cos, sin, wq, wk, wv]
        specs += [pl.BlockSpec((seg, d), lambda i: (0, 0)), pl.BlockSpec(g1.shape, lambda i: (0, 0)), cs, cs]
        specs += [pl.BlockSpec((None, d, TQ), lambda i, p=p: (lq, 0, clamp(i - npair - p * nq, nq))) for p in (2, 1, 0)]
        outs += [jax.ShapeDtypeStruct((ncp, seg, w), BF16)] * 3
        ospecs += [pl.BlockSpec((TQ // w, seg, w), lambda i, p=p: (clamp(i - npair - p * nq, nq), 0, 0)) for p in (2, 1, 0)]
        scratch = [pltpu.VMEM((seg, d), BF16)]
    out = pl.pallas_call(
        functools.partial(_attn_kernel, high, ncp, nq, lq, k),
        grid=(npair + 3 * nq,),
        in_specs=specs + [HBM] * k,
        out_specs=ospecs + [HBM] * k,
        out_shape=outs + [jax.ShapeDtypeStruct(a.shape, BF16) for a in send],
        scratch_shapes=scratch
        + [pltpu.VMEM((nh, c2, c2), F32), pltpu.VMEM((nh, 1, c2), F32), pltpu.VMEM((nh, HEAD + EXTRA, c2), F32),
           pltpu.VMEM((npair, c2, w), BF16), pltpu.SemaphoreType.DMA((ncp,)), pltpu.SemaphoreType.DMA((ncp,)),
           pltpu.SemaphoreType.DMA]
        + [pltpu.VMEM((nh, HEAD + EXTRA, rows), BF16)] * (len(kv) // 2) + _exchange_scratch(ncp, send),
        compiler_params=ids.params(True), name=('attn_high' if high else 'attn_low') + ('_qkv' if nq else ''),
    )(*args, *send)
    return out[:len(out) - k], out[len(out) - k:]


def _first_kernel(ncp, nq, x_ref, g1, cos, sin, wq, wk, wv, qh, kh, vh, ql, kl, vl, h_s, buf, ssem, rsem, lsem):
    i = pl.program_id(0)
    me = lax.axis_index('cp')
    req = lax.axis_index('req')
    seg = x_ref.shape[0] // 2
    wd = qh.shape[2]
    per = TN // wd

    @pl.when(i == 0)
    def _():
        _greet(ncp)
        h_s[...] = _norm(x_ref[...], g1[0:1])

    def remote(p, t, dst):
        return pltpu.make_async_remote_copy(buf.at[p, t], dst.at[me], ssem.at[p * ncp + t], rsem.at[p * ncp + me],
                                            device_id=(req, t), device_id_type=MESH)

    def own(p, dst):
        return pltpu.make_async_copy(buf.at[p, me], dst.at[me], lsem.at[p])

    def project(p, w, high, low, rope):
        n = i - p * nq
        t = jnp.dot(h_s[...], w[...], preferred_element_type=F32)
        for j in range(TN // HEAD):
            th = t[:, j * HEAD:(j + 1) * HEAD]
            if rope:
                th = th * cos[...] + pltpu.roll(th, HEAD // 2, 1) * sin[...]
            th = th.astype(BF16)
            lo = j * HEAD % wd
            e = j * HEAD // wd
            buf[p, per * n + e, :, lo:lo + HEAD] = th[:seg]
            high[e, :, lo:lo + HEAD] = th[seg:]
        for e in range(per):
            to = per * n + e

            @pl.when(to != me)
            def _():
                remote(p, to, low).start()

            @pl.when(to == me)
            def _():
                own(p, low).start()

    @pl.when(i < nq)
    def _():
        project(0, wv, vh, vl, False)

    @pl.when((i >= nq) & (i < 2 * nq))
    def _():
        project(1, wk, kh, kl, True)

    @pl.when(i >= 2 * nq)
    def _():
        project(2, wq, qh, ql, True)

    @pl.when(i == 3 * nq - 1)
    def _():
        for p, dst in enumerate((vl, kl, ql)):
            own(p, dst).wait()
            for o in range(1, ncp):
                t = lax.rem(me + o, ncp)
                remote(p, t, dst).wait_send()
                pltpu.make_async_remote_copy(buf.at[p, t], dst.at[t], ssem.at[p * ncp + t], rsem.at[p * ncp + t],
                                             device_id=(req, t), device_id_type=MESH).wait_recv()


def _first(ids, ncp, x, g1, cos, sin, wq, wk, wv):
    rows, d = x.shape
    seg, wd, nq = rows // 2, wq.shape[2] // ncp, wq.shape[2] // TN
    clamp = lambda v, n: jnp.clip(v, 0, n - 1)
    full = lambda a: pl.BlockSpec(a.shape, lambda i: (0, 0))
    blocks = jax.ShapeDtypeStruct((ncp, seg, wd), BF16)
    out = pl.pallas_call(
        functools.partial(_first_kernel, ncp, nq), grid=(3 * nq,),
        in_specs=[full(x), full(g1), full(cos), full(sin)]
        + [pl.BlockSpec((None, d, TN), lambda i, p=p: (0, 0, clamp(i - p * nq, nq))) for p in (2, 1, 0)],
        out_specs=[pl.BlockSpec((TN // wd, seg, wd), lambda i, p=p: (clamp(i - p * nq, nq), 0, 0)) for p in (2, 1, 0)] + [HBM] * 3,
        out_shape=[blocks] * 6,
        scratch_shapes=[pltpu.VMEM((rows, d), BF16), pltpu.VMEM((3, ncp, seg, wd), BF16), pltpu.SemaphoreType.DMA((3 * ncp,)),
                        pltpu.SemaphoreType.DMA((3 * ncp,)), pltpu.SemaphoreType.DMA((3,))],
        compiler_params=ids.params(True), name='first_qkv')(x, g1, cos, sin, wq, wk, wv)
    return out[:3], out[3:]


TO = 512
TF = 512
TQ = 1024
TN = 512


def _norm(x, g):
    x32 = x.astype(F32)
    r = lax.rsqrt(jnp.mean(x32 * x32, axis=-1, keepdims=True) + 1e-5)
    return (x32 * r * g.astype(F32)).astype(BF16)


def _dense_kernel(ncp, nm, nf, nq, lm, lq, cache, k, *refs):
    it = iter(refs)
    take = lambda n: [next(it) for _ in range(n)]
    x_ref, = take(1)
    if nm:
        o_ref, wo, g2, w1, w3, w2 = take(6)
    if nq:
        g1, cos, sin, wq, wk, wv = take(6)
    if cache:
        other, = take(1)
        land = take(8)
    srcs = take(k)
    if nm:
        y_ref, = take(1)
    if nq:
        qo, ko, vo = take(3)
    if cache:
        kc, vc = take(2)
    dsts = take(k)
    h_s, = take(1)
    if nm:
        o_s, x_s, acc = take(3)
    i = pl.program_id(0)
    last = nm + nf + 3 * nq - 1
    if k:
        ex = _Exchange(ncp, srcs, dsts, take(4), i == 0, i == 1, i == last)
        ex.begin()
    if nm:
        @pl.when(i == 0)
        def _():
            w = o_ref.shape[2]
            for j in range(ncp):
                o_s[:, j * w:(j + 1) * w] = o_ref[j]

        for j in range(nm):
            @pl.when(i == j)
            def _():
                ns = slice(j * TO, (j + 1) * TO)
                x_s[:, ns] = (x_ref[:, ns].astype(F32) + jnp.dot(
                    o_s[...], wo[...], preferred_element_type=F32)).astype(BF16)

        @pl.when(i == nm)
        def _():
            h_s[...] = _norm(x_s[...], g2[lm:lm + 1])
            acc[...] = jnp.zeros_like(acc)

        @pl.when((i >= nm) & (i < nm + nf))
        def _():
            h = h_s[...]
            a = jnp.dot(h, w1[...], preferred_element_type=F32)
            c = jnp.dot(h, w3[...], preferred_element_type=F32)
            u = (jax.nn.silu(a) * c).astype(BF16)
            acc[...] += jnp.dot(u, w2[...], preferred_element_type=F32)

        @pl.when(i == nm + nf - 1)
        def _():
            y = (x_s[...].astype(F32) + acc[...]).astype(BF16)
            seg = x_s.shape[0]
            if cache:
                y_ref[:seg] = other[...]
                y_ref[seg:] = y
            else:
                y_ref[...] = y
            if nq:
                x_s[...] = y
    if nq:
        s = i - (nm + nf)

        @pl.when(s == 0)
        def _():
            h_s[...] = _norm(x_s[...], g1[lq:lq + 1])

        _project(s, nq, h_s, (wq, wk, wv), cos, sin, (qo, ko, vo))
    if cache:
        s = i - nm
        half = cache // 2

        def put(out, l, src):
            out[l] = src[...].reshape(out.shape[1:])

        @pl.when((s >= 0) & (s < half))
        def _():
            for l in range(2):
                put(kc, l, land[l])
                put(vc, l, land[4 + l])

        @pl.when((s >= half) & (s < cache))
        def _():
            for l in range(2):
                put(kc, l, land[2 + l])
                put(vc, l, land[6 + l])
    if k:
        ex.end()


def _dense(ids, ncp, x, half, mlp=None, qkv=None, cache=None, send=()):
    d = x.shape[1]
    seg = x.shape[0] // 2 if half is not None else x.shape[0]
    hb = half or 0
    k = len(send)
    nm = nf = nq = l = lq = 0
    clamp = lambda v, n: jnp.clip(v, 0, n - 1)
    one = dict(pipeline_mode=pl.Buffered(1))
    xs = pl.BlockSpec((seg, d), lambda i: (hb, 0), **one)
    args, specs, outs, ospecs, scratch = [x], [xs], [], [], [pltpu.VMEM((seg, d), BF16)]
    if mlp is not None:
        l, o, wo, g2, w1, w3, w2 = mlp
        ff = w1.shape[2]
        tf = 2 * TF if qkv is None and cache is None else TF
        nm, nf = d // TO, ff // tf
        nm_, nf_ = nm, nf
        args += [o, wo, g2, w1, w3, w2]
        specs += [pl.BlockSpec(o.shape, lambda i: (0, 0, 0), **one),
                  pl.BlockSpec((None, d, TO), lambda i: (l, 0, clamp(i, nm_))),
                  pl.BlockSpec(g2.shape, lambda i: (0, 0)),
                  pl.BlockSpec((None, d, tf), lambda i: (l, 0, clamp(i - nm_, nf_))),
                  pl.BlockSpec((None, d, tf), lambda i: (l, 0, clamp(i - nm_, nf_))),
                  pl.BlockSpec((None, tf, d), lambda i: (l, clamp(i - nm_, nf_), 0))]
        scratch += [pltpu.VMEM((seg, d), BF16), pltpu.VMEM((seg, d), BF16), pltpu.VMEM((seg, d), F32)]
    base = nm + nf
    if qkv is not None:
        lq, g1, cos, sin, wq, wk, wv = qkv
        nq = wq.shape[2] // TQ
        nq_ = nq
        cs = pl.BlockSpec((seg, HEAD), lambda i: (hb, 0), **one)
        args += [g1, cos, sin, wq, wk, wv]
        specs += [pl.BlockSpec(g1.shape, lambda i: (0, 0)), cs, cs]
        specs += [pl.BlockSpec((None, d, TQ), lambda i, p=p: (lq, 0, clamp(i - base - p * nq_, nq_))) for p in (2, 1, 0)]
    if cache is not None:
        other, land = cache
        w = land[0].shape[2]
        args += [other] + list(land)
        lo = pl.BlockSpec((None, seg, w), lambda i: (clamp(i - nm_, ncp), 0, 0))
        hi = pl.BlockSpec((None, seg, w), lambda i: (ncp - 1 - clamp(i - nm_ - ncp, ncp), 0, 0))
        specs += [pl.BlockSpec((seg, d), lambda i: (0, 0), **one)] + [lo, lo, hi, hi] * 2
    args += list(send)
    specs += [HBM] * k
    if mlp is not None:
        ys = (2 * seg, d) if cache is not None else (seg, d)
        outs.append(jax.ShapeDtypeStruct(ys, BF16))
        ospecs.append(pl.BlockSpec(ys, lambda i: (0, 0)))
    if qkv is not None:
        wd = wq.shape[2] // ncp
        for p in (2, 1, 0):
            outs.append(jax.ShapeDtypeStruct((ncp, seg, wd), BF16))
            ospecs.append(pl.BlockSpec((TQ // wd, seg, wd), lambda i, p=p: (clamp(i - base - p * nq_, nq_), 0, 0)))
    if cache is not None:
        for _ in range(2):
            outs.append(jax.ShapeDtypeStruct((2, 2 * ncp * seg, w // HEAD, HEAD), BF16))
            ospecs.append(pl.BlockSpec((2, seg, w // HEAD, HEAD), lambda i: (0, clamp(i - nm_, 2 * ncp), 0, 0)))
    outs += [jax.ShapeDtypeStruct(a.shape, BF16) for a in send]
    ospecs += [HBM] * k
    out = pl.pallas_call(
        functools.partial(_dense_kernel, ncp, nm, nf, nq, l, lq, 2 * ncp if cache is not None else 0, k),
        grid=(nm + nf + 3 * nq,), in_specs=specs, out_specs=ospecs, out_shape=outs,
        scratch_shapes=scratch + _exchange_scratch(ncp, send), compiler_params=ids.params(k),
        name='dense' + ('_mlp' if nm else '') + ('_qkv' if nq else ''))(*args)
    return out[:len(out) - k], out[len(out) - k:]


def _project(s, nq, h_s, ws, cos, sin, outs):
    def project(w, out, rope):
        wd = out.shape[2]
        t = jnp.dot(h_s[...], w[...], preferred_element_type=F32)
        for c in range(0, TQ, HEAD):
            th = t[:, c:c + HEAD]
            if rope:
                th = th * cos[...] + pltpu.roll(th, HEAD // 2, 1) * sin[...]
            out[c // wd, :, c % wd:c % wd + HEAD] = th.astype(BF16)

    for n, p in enumerate((2, 1, 0)):
        @pl.when((s >= n * nq) & (s < (n + 1) * nq))
        def _():
            project(ws[p], outs[p], p < 2)


def _angles(pos):
    half = HEAD // 2
    inv = 1.0 / (10000.0 ** (jnp.arange(half, dtype=F32) * (2.0 / HEAD)))
    ang = pos.astype(F32)[:, None] * inv
    c, s = jnp.cos(ang), jnp.sin(ang)
    return jnp.concatenate([c, c], axis=-1), jnp.concatenate([-s, s], axis=-1)


def solution(mesh):
    ncp = mesh.shape['cp']
    act = P(('req', 'cp'), None)
    cache = P(None, 'req', 'cp', None)

    def body(x, pos, g1, g2, wq, wk, wv, wo, w1, w3, w2):
        ids = _Ids()
        cos, sin = _angles(pos)

        def mlp(l, o):
            return (l, o, wo, g2, w1, w3, w2)

        qkv = (1, g1, cos, sin, wq, wk, wv)
        dense = functools.partial(_dense, ids, ncp)
        a0h, (q, k0l, v0l) = _first(ids, ncp, x, g1, cos, sin, wq, wk, wv)
        (o,), _ = _attention(ids, q, (k0l, v0l))
        (xl, *a1l), (q, k0h, v0h) = dense(x, 0, mlp=mlp(0, o), qkv=qkv, send=tuple(a0h))
        (o,), (v1l,) = _attention(ids, q, (k0l, v0l, k0h, v0h), send=(a1l[2],))
        (xh,), (q, k1l) = dense(x, 1, mlp=mlp(0, o), send=(a1l[0], a1l[1]))
        (o, *a1h), _ = _attention(ids, q, (k1l, v1l), qkv=(xh, 1) + qkv)
        (xl,), (q, k1h, v1h) = dense(xl, None, mlp=mlp(1, o), send=tuple(a1h))
        (o,), _ = _attention(ids, q, (k1l, v1l, k1h, v1h))
        (y, kc, vc), _ = dense(xh, None, mlp=mlp(1, o), cache=(xl, (k0l, k1l, k0h, k1h, v0l, v1l, v0h, v1h)))
        return y, kc, vc

    return jax.shard_map(body, mesh=mesh, in_specs=(act, P(('req', 'cp'))) + (P(),) * 9,
                         out_specs=(act, cache, cache), check_vma=False)
```
